512 devices in a mesh: space: 64 (over z, x, core), chan: 8 (over y).
Axes of the slice: x: 4, y: 8, z: 8, core: 2. Of those that a mesh axis runs over, the one named last changes fastest.
Arguments:
- state: bfloat16 [384, 512, 1024], P('space', 'chan'), may hold values from -6 to 6
- cotangent: bfloat16 [384, 512, 1024], P('space', None, 'chan'), may hold values from -6 to 6
- order_table: int32 [384], replicated, may hold values from 0 to 383, as said below
- quad_weight: float32 [384], P('space'), may hold values from 0.5 to 2
- legendre: bfloat16 [384, 384, 384], P('space', 'chan'), as said below
- spec_gain: float32 [384, 512], P('chan'), may hold values from 0.5 to 2
- spectral_weight: bfloat16 [2, 512, 512], replicated, may hold values from -0.1875 to 0.1875
- mlp_in: bfloat16 [512, 768], P('chan'), may hold values from -0.25 to 0.25
- mlp_out: bfloat16 [768, 512], P('chan'), may hold values from -0.21875 to 0.21875
Outputs:
- output: bfloat16 [384, 512, 1024], P('space', None, 'chan')
- state_grad: bfloat16 [384, 512, 1024], P('space', 'chan')
The draws below stay inside these ranges and needn't reach their ends.
Inputs may be any that keep to these rules, and one draw needn't show every extreme that they name: order_table holds each of 0 to 383 once; slots 2 j and 2 j + 1 hold orders m and 383 - m with m < 192. legendre[k, l, t] is zero for every degree l below order_table[k].
All inputs are finite; a program needn't handle non-finite values.
Results may differ from the reference program's by a relative error of at most 0.015.
Values may be sent and summed in bfloat16 or wider, within the bound.
No kernel may reach another device: no remote copies, remote signals or barrier semaphores. Data moves between devices by JAX's collectives and lax.ppermute only.
A program may use at most 64 MiB of HBM per device.

```python
import math
import jax
import jax.numpy as jnp
from jax import lax

C = 512
H = 768
NLON = 1024
NLAT = 384
M = 384


def pairing(key):
    shuffled = jax.random.permutation(jax.random.fold_in(key, 11), M // 2).astype(jnp.int32)
    return jnp.stack([shuffled, M - 1 - shuffled], axis=1).reshape(M).astype(jnp.int32)


def draw_order_table(key, part):
    return pairing(key)


def draw_legendre(key, part):
    orders = pairing(key)
    degree = lax.broadcasted_iota(jnp.int32, (M, M, NLAT), 1)
    live = degree >= orders[:, None, None]
    value_key = jax.random.fold_in(key, 23)
    values = jax.random.normal(value_key, (M, M, NLAT), jnp.float32)
    scaled = jnp.where(live, values, 0.0) * (1.0 / NLAT) ** 0.5
    return scaled.astype(jnp.bfloat16)


def block_levels(own_key, shape, cuts, low, high):
    def one(position, parts):
        draws = jax.random.uniform(jax.random.fold_in(jax.random.fold_in(own_key, 6), position), (parts,), jnp.float32, low / len(cuts), high / len(cuts))
        return jnp.repeat(jnp.exp(draws), shape[position] // parts).reshape((-1,) + (1,) * (len(shape) - position - 1))

    loudness = one(*cuts[0])
    for cut in cuts[1:]:
        loudness = loudness * one(*cut)
    return loudness


def scatter_about(key, shape, width, limit, shards=(), held_as=jnp.bfloat16):
    result = jax.random.normal(key, shape, jnp.float32) * width
    if len(shards) > 0:
        result = block_levels(key, shape, shards, -0.22, 0.18) * result
    return jnp.clip(result, min=-limit, max=limit).astype(held_as)


def setup_inputs(seed: int = 0) -> dict:
    splits = jax.random.split(jax.random.key(seed), 10)
    return {
        "state": scatter_about(splits[0], (NLAT, C, NLON), 1.0, 6.0, ((0, 64), (1, 8))),
        "cotangent": scatter_about(splits[1], (NLAT, C, NLON), 1.0, 6.0, ((0, 64), (2, 8))),
        "order_table": draw_order_table(jax.random.fold_in(splits[9], 71), 0),
        "quad_weight": jnp.clip(jnp.exp(math.log(2.0) - 1.3862944 * jax.random.uniform(splits[3], (NLAT,), jnp.float32) ** block_levels(splits[3], (NLAT,), ((0, 64),), -0.2, 0.2)), 0.5, 2.0),
        "legendre": draw_legendre(jax.random.fold_in(splits[9], 71), 0),
        "spec_gain": jnp.clip(jnp.exp(math.log(2.0) - 1.3862944 * jax.random.uniform(splits[5], (M, C), jnp.float32) ** block_levels(splits[5], (M, C), ((0, 8),), -0.2, 0.2)), 0.5, 2.0),
        "spectral_weight": scatter_about(splits[6], (2, C, C), (2 * C) ** -0.5, 0.1875),
        "mlp_in": scatter_about(splits[7], (C, H), C ** -0.5, 0.25, ((0, 8),)),
        "mlp_out": scatter_about(splits[8], (H, C), H ** -0.5, 0.21875, ((0, 8),)),
    }


def transform_tables(order_table, lon_count):
    points = lax.broadcasted_iota(jnp.int32, (lon_count, order_table.shape[0]), 0)
    phases = points * order_table.astype(jnp.int32)[None, :] % lon_count
    angles = phases.astype(jnp.float32) * (2.0 * math.pi / lon_count)
    factor = 1.0 / math.sqrt(lon_count)
    forward = jnp.stack([jnp.cos(angles), -jnp.sin(angles)], axis=2) * factor
    weighting = jnp.where(order_table == 0, 1.0, 2.0).astype(jnp.float32)
    inverse = forward * weighting[None, :, None]
    return (forward.reshape(lon_count, -1).astype(jnp.bfloat16), inverse.reshape(lon_count, -1).astype(jnp.bfloat16))

def rounded(values):
    return lax.optimization_barrier(values.astype(jnp.bfloat16))

def mlp_row(row_pair, mlp_in, mlp_out):
    hidden_row, cot_row = row_pair
    first_layer = mlp_in.astype(jnp.float32)
    second_layer = mlp_out.astype(jnp.float32)
    pre_act = jnp.einsum('cn,ch->hn', hidden_row.astype(jnp.float32), first_layer)
    active = rounded(jax.nn.gelu(pre_act)).astype(jnp.float32)
    output_row = (hidden_row.astype(jnp.float32) + jnp.einsum('hn,hc->cn', active, second_layer)).astype(jnp.bfloat16)
    back_hidden = jnp.einsum('cn,hc->hn', cot_row.astype(jnp.float32), second_layer)
    pullback = jax.vjp(jax.nn.gelu, pre_act)[1]
    inner_grad = rounded(pullback(back_hidden)[0]).astype(jnp.float32)
    grad_row = (cot_row.astype(jnp.float32) + jnp.einsum('hn,ch->cn', inner_grad, first_layer)).astype(jnp.bfloat16)
    return (output_row, grad_row)

def reference(state, cotangent, order_table, quad_weight, legendre, spec_gain, spectral_weight, mlp_in, mlp_out):
    forward_table, inverse_table = transform_tables(order_table, NLON)
    forward_grid = forward_table.astype(jnp.float32).reshape(NLON, M, 2)
    inverse_grid = inverse_table.astype(jnp.float32).reshape(NLON, M, 2)
    legend = legendre.astype(jnp.float32)
    weight_real = spectral_weight[0].astype(jnp.float32)
    weight_imag = spectral_weight[1].astype(jnp.float32)
    gains = spec_gain[:, None, :]
    spectral = rounded(jnp.einsum('tcn,nkr->tkrc', state.astype(jnp.float32), forward_grid) * quad_weight[:, None, None, None])
    coeffs = rounded(jnp.einsum('klt,tkrc->lkrc', legend, spectral.astype(jnp.float32)))
    coeff_real = coeffs[:, :, 0].astype(jnp.float32)
    coeff_imag = coeffs[:, :, 1].astype(jnp.float32)
    mixed_real = (jnp.einsum('lkc,co->lko', coeff_real, weight_real) - jnp.einsum('lkc,co->lko', coeff_imag, weight_imag)) * gains
    mixed_imag = (jnp.einsum('lkc,co->lko', coeff_real, weight_imag) + jnp.einsum('lkc,co->lko', coeff_imag, weight_real)) * gains
    mixed = rounded(jnp.stack([mixed_real, mixed_imag], axis=2))
    synth = rounded(jnp.einsum('klt,lkrc->tkrc', legend, mixed.astype(jnp.float32)))
    wave = jnp.einsum('tkrc,nkr->tcn', synth.astype(jnp.float32), inverse_grid)
    hidden = rounded(state.astype(jnp.float32) + wave)
    output, hidden_grad = lax.map(lambda row_pair: mlp_row(row_pair, mlp_in, mlp_out), (hidden, cotangent))
    back_spec = rounded(jnp.einsum('tcn,nkr->tkrc', hidden_grad.astype(jnp.float32), inverse_grid))
    back_coeff = rounded(jnp.einsum('klt,tkrc->lkrc', legend, back_spec.astype(jnp.float32)))
    scaled_real = rounded(back_coeff[:, :, 0].astype(jnp.float32) * gains).astype(jnp.float32)
    scaled_imag = rounded(back_coeff[:, :, 1].astype(jnp.float32) * gains).astype(jnp.float32)
    back_real = jnp.einsum('lko,co->lkc', scaled_real, weight_real) + jnp.einsum('lko,co->lkc', scaled_imag, weight_imag)
    back_imag = jnp.einsum('lko,co->lkc', scaled_imag, weight_real) - jnp.einsum('lko,co->lkc', scaled_real, weight_imag)
    back_mixed = rounded(jnp.stack([back_real, back_imag], axis=2))
    back_field = rounded(jnp.einsum('klt,lkrc->tkrc', legend, back_mixed.astype(jnp.float32)))
    field_grad = jnp.einsum('tkrc,nkr->tcn', back_field.astype(jnp.float32), forward_grid) * quad_weight[:, None, None]
    state_grad = (hidden_grad.astype(jnp.float32) + field_grad).astype(jnp.bfloat16)
    return (output, state_grad)
```

```python
import functools
import math

import jax
import jax.numpy as jnp
from jax import lax
from jax.experimental import pallas as pl
from jax.experimental.pallas import tpu as pltpu
from jax.sharding import PartitionSpec as P

BF = jnp.bfloat16
F32 = jnp.float32
LAT = 6
WIDE = 64
LANES = 128
VMEM_LIMIT = 28 * 1024 * 1024


def rows_dot(a, b):
    return lax.dot_general(a, b, (((1,), (0,)), ((), ())), preferred_element_type=F32)


def lanes_dot(a, b):
    return lax.dot_general(a, b, (((1,), (1,)), ((), ())), preferred_element_type=F32)


def heads_dot(a, b):
    return lax.dot_general(a, b, (((0,), (0,)), ((), ())), preferred_element_type=F32)


def interleaver():
    size = LANES * LAT
    row = lax.broadcasted_iota(jnp.int32, (size, size), 0)
    col = lax.broadcasted_iota(jnp.int32, (size, size), 1)
    wanted = (col & (LANES - 1)) * LAT + (col >> 7)
    return jnp.where(row == wanted, 1.0, 0.0).astype(BF)


def by_latitude(values, factor):
    pieces = [values[t * WIDE : (t + 1) * WIDE] * factor(t) for t in range(LAT)]
    return jnp.concatenate(pieces, axis=0)


def send_orders(spec, mover, send_ref):
    half = spec.shape[1] // 2
    for q in range(half // LANES):
        pieces = []
        for t in range(LAT):
            rows = spec[t * WIDE : (t + 1) * WIDE]
            real = rows[:, q * LANES : (q + 1) * LANES]
            imag = rows[:, half + q * LANES : half + (q + 1) * LANES]
            pieces.append(jnp.concatenate([real, imag], axis=0))
        block = jnp.concatenate(pieces, axis=1)
        step = LANES * LAT
        send_ref[q * step : (q + 1) * step, :] = lanes_dot(mover, block).astype(BF)


def take_orders(recv_ref, mover, half):
    step = LANES * LAT
    blocks = []
    for q in range(half // LANES):
        blocks.append(heads_dot(recv_ref[q * step : (q + 1) * step, :], mover).astype(BF))
    bands = []
    for t in range(LAT):
        lanes = slice(t * LANES, (t + 1) * LANES)
        real = [b[:WIDE, lanes] for b in blocks]
        imag = [b[WIDE:, lanes] for b in blocks]
        bands.append(jnp.concatenate(real + imag, axis=1))
    return jnp.concatenate(bands, axis=0)


def side_by_side(ref):
    return jnp.concatenate([ref[i] for i in range(ref.shape[0])], axis=1)


def pack_kernel(legendre_ref, gain_ref, in_ref, out_ref, table_ref, layers_ref):
    slots = legendre_ref.shape[0]
    lats = legendre_ref.shape[2]
    table_ref[:slots] = legendre_ref[...]
    gain = gain_ref[...].astype(BF)
    rest = gain.shape[1] - lats
    table_ref[slots] = gain[:, :lats]
    table_ref[slots + 1, :, :rest] = gain[:, lats:]
    rows, width = in_ref.shape
    lanes = out_ref.shape[1]
    over = width - lanes
    layers_ref[:rows] = in_ref[:, :lanes]
    layers_ref[rows : rows + rows // 2, :over] = in_ref[: rows // 2, lanes:]
    layers_ref[rows : rows + rows // 2, over:] = in_ref[rows // 2 :, lanes:]
    layers_ref[rows + rows // 2 :] = out_ref[...]


def weight_kernel(spectral_ref, weight_ref):
    real, imag = spectral_ref[0], spectral_ref[1]
    groups = real.shape[1] // WIDE

    def paired(left, right):
        pieces = []
        for i in range(groups):
            lanes = slice(i * WIDE, (i + 1) * WIDE)
            pieces += [left[:, lanes], right[:, lanes]]
        return jnp.concatenate(pieces, axis=1)

    for at, rows in enumerate((paired(real, imag), paired(-imag, real))):
        for i in range(groups):
            start = (2 * i + at) * WIDE
            weight_ref[start : start + WIDE] = rows[i * WIDE : (i + 1) * WIDE]


def dft_kernel(quad_ref, order_ref, state_ref, table_ref, mover_ref, send_ref):
    slots = order_ref.shape[1]
    lon_count = state_ref.shape[1]
    spaces = slots // LAT
    place = lax.broadcasted_iota(jnp.int32, (slots, slots), 0)
    wanted = (place & (spaces - 1)) * LAT + place // spaces
    lane = lax.broadcasted_iota(jnp.int32, (slots, slots), 1)
    picked = jnp.where(lane == wanted, order_ref[...].astype(F32), 0.0)
    orders = jnp.sum(picked, axis=1, keepdims=True).astype(jnp.int32)
    points = lax.broadcasted_iota(jnp.int32, (slots, LANES), 1)
    step = 2.0 * math.pi / lon_count
    factor = 1.0 / math.sqrt(lon_count)
    angles = ((points * orders) & (lon_count - 1)).astype(F32) * step
    turns = ((jnp.full_like(points, LANES) * orders) & (lon_count - 1)).astype(F32) * step
    cosine, sine = jnp.cos(angles) * factor, jnp.sin(angles) * factor
    turn_cos, turn_sin = jnp.cos(turns), jnp.sin(turns)
    for a in range(lon_count // LANES):
        lanes = slice(a * LANES, (a + 1) * LANES)
        table_ref[:slots, lanes] = cosine.astype(BF)
        table_ref[slots:, lanes] = (-sine).astype(BF)
        cosine, sine = (
            cosine * turn_cos - sine * turn_sin,
            sine * turn_cos + cosine * turn_sin,
        )
    mover_ref[...] = interleaver()
    spec = lanes_dot(state_ref[...], table_ref[...])
    spec = by_latitude(spec, lambda t: quad_ref[t]).astype(BF)
    send_orders(spec, mover_ref[...], send_ref)


def slot_tables(own_ref, gathered_ref):
    groups, slots = gathered_ref.shape[0], gathered_ref.shape[1] - 2
    own = own_ref[1]
    legendre = jnp.concatenate([gathered_ref[i, own] for i in range(groups)], axis=0)
    low = jnp.concatenate([gathered_ref[i, slots] for i in range(groups)], axis=0)
    high = jnp.concatenate([gathered_ref[i, slots + 1, :, :LANES] for i in range(groups)], axis=0)
    gain = jnp.concatenate([low, high], axis=1).astype(F32)
    wide = []
    for i in range(gain.shape[1] // WIDE):
        piece = gain[:, i * WIDE : (i + 1) * WIDE]
        wide.append(jnp.concatenate([piece, piece], axis=1))
    return legendre, wide


def slot_scale(own_ref, order_ref):
    return jnp.where(order_ref[own_ref[0]] == 0, 1.0, 2.0).astype(F32)


def slot_kernel(own_ref, order_ref, recv_ref, gathered_ref, weight_ref, send_ref):
    scale = slot_scale(own_ref, order_ref)
    legendre, gain = slot_tables(own_ref, gathered_ref)
    coeffs = rows_dot(legendre, side_by_side(recv_ref)).astype(BF)
    mixed = rows_dot(coeffs, weight_ref[...])
    parts = [
        (mixed[:, i * LANES : (i + 1) * LANES] * gain[i]).astype(BF) for i in range(len(gain))
    ]
    synth = heads_dot(legendre, jnp.concatenate(parts, axis=1)) * scale
    for i in range(len(gain)):
        send_ref[i] = synth[:, i * LANES : (i + 1) * LANES].astype(BF)


def back_slot_kernel(own_ref, order_ref, recv_ref, gathered_ref, weight_ref, send_ref):
    scale = slot_scale(own_ref, order_ref)
    legendre, gain = slot_tables(own_ref, gathered_ref)
    coeffs = (rows_dot(legendre, side_by_side(recv_ref)) * scale).astype(BF).astype(F32)
    scaled = [
        (coeffs[:, i * LANES : (i + 1) * LANES] * gain[i]).astype(BF) for i in range(len(gain))
    ]
    mixed = lanes_dot(jnp.concatenate(scaled, axis=1), weight_ref[...]).astype(BF)
    field = heads_dot(legendre, mixed).astype(BF)
    for i in range(len(gain)):
        send_ref[i] = field[:, i * LANES : (i + 1) * LANES]


def hidden_kernel(recv_ref, table_ref, mover_ref, state_ref, hidden_ref):
    field = take_orders(recv_ref, mover_ref[...], table_ref.shape[0] // 2)
    wave = rows_dot(field, table_ref[...])
    hidden = (state_ref[...].astype(F32) + wave).astype(BF)
    for i in range(hidden_ref.shape[0]):
        hidden_ref[i] = hidden[:, i * LANES : (i + 1) * LANES]


def mlp_kernel(hidden_ref, cot_ref, layers_ref, output_ref, grad_ref):
    groups = hidden_ref.shape[0]
    left, right, second = [], [], []
    half, over = WIDE // 2, layers_ref.shape[2] // 2
    for i in range(groups):
        left.append(layers_ref[i, :WIDE])
        right.append(layers_ref[i, WIDE : WIDE + half, :over])
        right.append(layers_ref[i, WIDE : WIDE + half, over:])
        second.append(layers_ref[i, WIDE + half :])
    left, right = jnp.concatenate(left, axis=0), jnp.concatenate(right, axis=0)
    first = jnp.concatenate([left, right], axis=1)
    second = jnp.concatenate(second, axis=0)
    root = math.sqrt(2.0 / math.pi)
    for pair in range(0, LAT, 2):
        hiddens, cots = [], []
        for t in (pair, pair + 1):
            rows = slice(t * WIDE, (t + 1) * WIDE)
            hiddens.append(jnp.concatenate([hidden_ref[i, rows] for i in range(groups)], axis=0))
            cots.append(cot_ref[t])
        hidden = jnp.concatenate(hiddens, axis=1)
        cot = jnp.concatenate(cots, axis=1)
        x = heads_dot(first, hidden)
        back = rows_dot(second, cot)
        square = x * x
        bend = jnp.tanh(root * x * (1.0 + 0.044715 * square))
        half = 0.5 + 0.5 * bend
        slope = half + 0.5 * x * (1.0 - bend * bend) * (root * (1.0 + 3 * 0.044715 * square))
        inner = (slope * back).astype(BF)
        active = (x * half).astype(BF)
        grad = (cot.astype(F32) + rows_dot(first, inner)).astype(BF)
        output = (hidden.astype(F32) + heads_dot(second, active)).astype(BF)
        for at, t in enumerate((pair, pair + 1)):
            lanes = slice(at * LANES, (at + 1) * LANES)
            output_ref[t] = output[:, lanes]
            for i in range(groups):
                grad_ref[i, t * WIDE : (t + 1) * WIDE, :] = grad[i * WIDE : (i + 1) * WIDE, lanes]


def back_dft_kernel(grad_ref, table_ref, mover_ref, send_ref):
    spec = lanes_dot(side_by_side(grad_ref), table_ref[...]).astype(BF)
    send_orders(spec, mover_ref[...], send_ref)


def state_grad_kernel(quad_ref, recv_ref, table_ref, mover_ref, grad_ref, out_ref):
    field = take_orders(recv_ref, mover_ref[...], table_ref.shape[0] // 2)
    wave = rows_dot(field, table_ref[...])
    wave = by_latitude(wave, lambda t: quad_ref[t])
    out_ref[...] = (side_by_side(grad_ref).astype(F32) + wave).astype(BF)


def call(kernel, outs, scalars, arrays, flops, name):
    out_shape = [jax.ShapeDtypeStruct(s, d) for s, d in outs]
    vmem = pl.BlockSpec(memory_space=pltpu.VMEM)
    smem = pl.BlockSpec(memory_space=pltpu.SMEM)
    single = len(outs) == 1
    moved = sum(a.size * a.dtype.itemsize for a in arrays)
    return pl.pallas_call(
        kernel,
        out_shape=out_shape[0] if single else out_shape,
        in_specs=[smem] * len(scalars) + [vmem] * len(arrays),
        out_specs=vmem if single else [vmem] * len(outs),
        compiler_params=pltpu.CompilerParams(vmem_limit_bytes=VMEM_LIMIT),
        cost_estimate=pl.CostEstimate(flops=flops, bytes_accessed=moved, transcendentals=0),
        name=name,
    )(*scalars, *arrays)


def shards(
    state,
    cotangent,
    order_table,
    quad_weight,
    legendre,
    spec_gain,
    spectral_weight,
    mlp_in,
    mlp_out,
):
    lat_rows, chan_width, lon_count = state.shape
    order_count = order_table.shape[0]
    slot_count, degree_rows, lat_count = legendre.shape
    space_count, chan_count = lax.axis_size("space"), lax.axis_size("chan")
    devices = space_count * chan_count
    channels = chan_count * chan_width
    both = ("chan", "space")

    def exchange(rows):
        pieces = rows.reshape(devices * lat_rows // 2, 2, LANES)
        moved = lax.all_to_all(pieces, both, split_axis=0, concat_axis=0, tiled=True)
        return moved.reshape(devices * lat_rows, LANES)

    def cross(blocks):
        return lax.all_to_all(blocks, "chan", split_axis=0, concat_axis=0, tiled=True)

    space_at, chan_at = lax.axis_index("space"), lax.axis_index("chan")
    own_row = jnp.minimum(chan_at, slot_count - 1)
    own = jnp.stack([space_at * slot_count + own_row, own_row])

    packed, layers = call(
        pack_kernel,
        [
            ((slot_count + 2, degree_rows, lat_count), BF),
            ((mlp_in.shape[0] * 3 // 2 + mlp_out.shape[0], mlp_out.shape[1]), BF),
        ],
        [],
        [legendre, spec_gain, mlp_in, mlp_out],
        1000,
        "pack",
    )
    tables = lax.all_gather(packed, "chan", axis=0)
    all_layers = lax.all_gather(layers, "chan", axis=0)
    weight = call(
        weight_kernel,
        [((2 * channels, 2 * channels), BF)],
        [],
        [spectral_weight],
        2 * 10**9,
        "weight",
    )

    flat = (lat_rows * chan_width, lon_count)
    send = (devices * lat_rows, LANES)
    table_shape = (2 * order_count, lon_count)
    blocks = (chan_count, lat_rows * chan_width, LANES)
    slot_shape = (chan_count, lat_count, LANES)
    dft_flops = 2 * 2 * order_count * lat_rows * chan_width * lon_count
    slot_flops = 2 * order_count * 2 * channels * (2 * lat_count + 2 * channels)
    flat_state = state.reshape(flat)

    table, mover, sent = call(
        dft_kernel,
        [(table_shape, BF), ((LANES * lat_rows, LANES * lat_rows), BF), (send, BF)],
        [quad_weight],
        [order_table.reshape(1, order_count), flat_state],
        dft_flops,
        "dft",
    )
    received = exchange(sent).reshape(slot_shape)
    sent = call(
        slot_kernel,
        [(slot_shape, BF)],
        [own, order_table],
        [received, tables, weight],
        slot_flops,
        "slot",
    )
    received = exchange(sent.reshape(send))
    hidden = call(
        hidden_kernel,
        [(blocks, BF)],
        [],
        [received, table, mover, flat_state],
        dft_flops,
        "hidden",
    )
    point_hidden = cross(hidden)
    output, point_grad = call(
        mlp_kernel,
        [(cotangent.shape, BF), (blocks, BF)],
        [],
        [point_hidden, cotangent, all_layers],
        4 * dft_flops,
        "mlp",
    )
    hidden_grad = cross(point_grad)
    sent = call(
        back_dft_kernel, [(send, BF)], [], [hidden_grad, table, mover], dft_flops, "back_dft"
    )
    received = exchange(sent).reshape(slot_shape)
    sent = call(
        back_slot_kernel,
        [(slot_shape, BF)],
        [own, order_table],
        [received, tables, weight],
        slot_flops,
        "back_slot",
    )
    received = exchange(sent.reshape(send))
    state_grad = call(
        state_grad_kernel,
        [(flat, BF)],
        [quad_weight],
        [received, table, mover, hidden_grad],
        dft_flops,
        "state_grad",
    )
    return (output, state_grad.reshape(state.shape))


def solution(mesh):
    placed = (
        P("space", "chan", None),
        P("space", None, "chan"),
        P(),
        P("space"),
        P("space", "chan", None),
        P("chan", None),
        P(),
        P("chan", None),
        P("chan", None),
    )
    return jax.shard_map(
        shards,
        mesh=mesh,
        in_specs=placed,
        out_specs=(P("space", None, "chan"), P("space", "chan", None)),
        check_vma=False,
    )
```

```python
import functools
import math

import jax
import jax.numpy as jnp
from jax import lax
from jax.experimental import pallas as pl
from jax.experimental.pallas import tpu as pltpu
from jax.sharding import PartitionSpec as P

BF = jnp.bfloat16
F32 = jnp.float32
LAT = 6
WIDE = 64
LANES = 128
UNIT = 16
VMEM_LIMIT = 28 * 1024 * 1024


def rows_dot(a, b):
    return lax.dot_general(a, b, (((1,), (0,)), ((), ())), preferred_element_type=F32)


def lanes_dot(a, b):
    return lax.dot_general(a, b, (((1,), (1,)), ((), ())), preferred_element_type=F32)


def heads_dot(a, b):
    return lax.dot_general(a, b, (((0,), (0,)), ((), ())), preferred_element_type=F32)


def interleaver():
    size = LANES * LAT
    row = lax.broadcasted_iota(jnp.int32, (size, size), 0)
    col = lax.broadcasted_iota(jnp.int32, (size, size), 1)
    wanted = (col & (LANES - 1)) * LAT + (col >> 7)
    return jnp.where(row == wanted, 1.0, 0.0).astype(BF)


def by_latitude(values, factor):
    pieces = [values[t * WIDE : (t + 1) * WIDE] * factor(t) for t in range(LAT)]
    return jnp.concatenate(pieces, axis=0)


def send_orders(spec, mover, send_ref):
    half = spec.shape[1] // 2
    for q in range(half // LANES):
        pieces = []
        for t in range(LAT):
            rows = spec[t * WIDE : (t + 1) * WIDE]
            real = rows[:, q * LANES : (q + 1) * LANES]
            imag = rows[:, half + q * LANES : half + (q + 1) * LANES]
            pieces.append(jnp.concatenate([real, imag], axis=0))
        block = jnp.concatenate(pieces, axis=1)
        step = LANES * LAT
        send_ref[q * step : (q + 1) * step, :] = lanes_dot(mover, block).astype(BF)


def take_orders(recv_ref, mover, half):
    step = LANES * LAT
    blocks = []
    for q in range(half // LANES):
        blocks.append(heads_dot(recv_ref[q * step : (q + 1) * step, :], mover).astype(BF))
    bands = []
    for t in range(LAT):
        lanes = slice(t * LANES, (t + 1) * LANES)
        real = [b[:WIDE, lanes] for b in blocks]
        imag = [b[WIDE:, lanes] for b in blocks]
        bands.append(jnp.concatenate(real + imag, axis=1))
    return jnp.concatenate(bands, axis=0)


def side_by_side(ref):
    return jnp.concatenate([ref[i] for i in range(ref.shape[0])], axis=1)


def pack_kernel(legendre_ref, gain_ref, in_ref, out_ref, table_ref, layers_ref):
    units, lats = legendre_ref.shape[0], table_ref.shape[2]
    rows, width = in_ref.shape
    lanes = out_ref.shape[1]
    over, half = width - lanes, rows // 2
    table_ref[:units] = legendre_ref[...]
    gain = gain_ref[...].astype(BF)
    count = gain.shape[0] // UNIT
    for i in range(count):
        own = slice(i * UNIT, (i + 1) * UNIT)
        table_ref[units + i] = gain[own, :lats]
        table_ref[units + count, :, i * LANES : (i + 1) * LANES] = gain[own, lats:]
    layers_ref[:rows] = in_ref[:, :lanes]
    layers_ref[rows : rows + half, :over] = in_ref[:half, lanes:]
    layers_ref[rows : rows + half, over:] = in_ref[half:, lanes:]
    layers_ref[rows + half :] = out_ref[...]


def build_weight(spectral_ref, weight_ref):
    real, imag = spectral_ref[0], spectral_ref[1]
    groups = real.shape[1] // WIDE

    def paired(left, right):
        pieces = []
        for i in range(groups):
            lanes = slice(i * WIDE, (i + 1) * WIDE)
            pieces += [left[:, lanes], right[:, lanes]]
        return jnp.concatenate(pieces, axis=1)

    for at, rows in enumerate((paired(real, imag), paired(-imag, real))):
        for i in range(groups):
            start = (2 * i + at) * WIDE
            weight_ref[start : start + WIDE] = rows[i * WIDE : (i + 1) * WIDE]


def dft_kernel(order_ref, state_ref, table_ref, mover_ref, send_ref):
    slots = table_ref.shape[0] // 2
    lon_count = state_ref.shape[1]
    spaces = slots // LAT
    place = lax.broadcasted_iota(jnp.int32, (slots, slots), 0)
    wanted = (place & (spaces - 1)) * LAT + place // spaces
    lane = lax.broadcasted_iota(jnp.int32, (slots, slots), 1)
    picked = jnp.where(lane == wanted, order_ref[:, :slots], 0.0)
    orders = jnp.sum(picked, axis=1, keepdims=True).astype(jnp.int32)
    points = lax.broadcasted_iota(jnp.int32, (slots, LANES), 1)
    step = 2.0 * math.pi / lon_count
    factor = 1.0 / math.sqrt(lon_count)
    angles = ((points * orders) & (lon_count - 1)).astype(F32) * step
    turns = ((jnp.full_like(points, LANES) * orders) & (lon_count - 1)).astype(F32) * step
    cosine, sine = jnp.cos(angles) * factor, jnp.sin(angles) * factor
    turn_cos, turn_sin = jnp.cos(turns), jnp.sin(turns)
    for a in range(lon_count // LANES):
        lanes = slice(a * LANES, (a + 1) * LANES)
        table_ref[:slots, lanes] = cosine.astype(BF)
        table_ref[slots:, lanes] = (-sine).astype(BF)
        cosine, sine = (
            cosine * turn_cos - sine * turn_sin,
            sine * turn_cos + cosine * turn_sin,
        )
    mover_ref[...] = interleaver()
    spec = lanes_dot(state_ref[...], table_ref[...])
    spec = by_latitude(spec, lambda t: order_ref[:, slots + t : slots + t + 1]).astype(BF)
    send_orders(spec, mover_ref[...], send_ref)


def both_parts(gain):
    wide = []
    for i in range(gain.shape[1] // WIDE):
        piece = gain[:, i * WIDE : (i + 1) * WIDE].astype(F32)
        wide.append(jnp.concatenate([piece, piece], axis=1))
    return wide


def slot_scale(own_ref, order_ref):
    return jnp.where(order_ref[own_ref[0]] == 0, 1.0, 2.0).astype(F32)


def slot_kernel(
    own_ref, order_ref, recv_ref, gathered_ref, weight_ref, send_ref, legendre_ref, gain_ref
):
    groups, count = gathered_ref.shape[0], legendre_ref.shape[0] // gathered_ref.shape[0] // UNIT
    units = gathered_ref.shape[1]
    first = own_ref[1] * count
    scale = slot_scale(own_ref, order_ref)
    rows = [gathered_ref[i, first + u] for i in range(groups) for u in range(count)]
    legendre = jnp.concatenate(rows, axis=0)
    legendre_ref[...] = legendre
    coeffs = rows_dot(legendre, side_by_side(recv_ref)).astype(BF)
    low = [gathered_ref[i, units - 1 - count + u] for i in range(groups) for u in range(count)]
    high = [
        gathered_ref[i, units - 1, :, u * LANES : (u + 1) * LANES]
        for i in range(groups)
        for u in range(count)
    ]
    gain = jnp.concatenate([jnp.concatenate(low, axis=0), jnp.concatenate(high, axis=0)], axis=1)
    gain_ref[...] = gain
    wide = both_parts(gain)
    mixed = rows_dot(coeffs, weight_ref[...])
    parts = [
        (mixed[:, i * LANES : (i + 1) * LANES] * wide[i]).astype(BF) for i in range(len(wide))
    ]
    synth = heads_dot(legendre, jnp.concatenate(parts, axis=1)) * scale
    for i in range(len(wide)):
        send_ref[i] = synth[:, i * LANES : (i + 1) * LANES].astype(BF)


def back_slot_kernel(
    own_ref, order_ref, recv_ref, legendre_ref, gain_ref, spectral_ref, send_ref, weight_ref
):
    build_weight(spectral_ref, weight_ref)
    scale = slot_scale(own_ref, order_ref)
    legendre, wide = legendre_ref[...], both_parts(gain_ref[...])
    coeffs = (rows_dot(legendre, side_by_side(recv_ref)) * scale).astype(BF).astype(F32)
    scaled = [
        (coeffs[:, i * LANES : (i + 1) * LANES] * wide[i]).astype(BF) for i in range(len(wide))
    ]
    mixed = lanes_dot(jnp.concatenate(scaled, axis=1), weight_ref[...]).astype(BF)
    field = heads_dot(legendre, mixed).astype(BF)
    for i in range(len(wide)):
        send_ref[i] = field[:, i * LANES : (i + 1) * LANES]


def hidden_kernel(recv_ref, table_ref, mover_ref, state_ref, hidden_ref):
    field = take_orders(recv_ref, mover_ref[...], table_ref.shape[0] // 2)
    wave = rows_dot(field, table_ref[...])
    hidden = (state_ref[...].astype(F32) + wave).astype(BF)
    for i in range(hidden_ref.shape[0]):
        hidden_ref[i] = hidden[:, i * LANES : (i + 1) * LANES]


def mlp_kernel(hidden_ref, cot_ref, layers_ref, output_ref, grad_ref):
    groups = hidden_ref.shape[0]
    left, right, second = [], [], []
    half, over = WIDE // 2, layers_ref.shape[2] // 2
    for i in range(groups):
        left.append(layers_ref[i, :WIDE])
        right.append(layers_ref[i, WIDE : WIDE + half, :over])
        right.append(layers_ref[i, WIDE : WIDE + half, over:])
        second.append(layers_ref[i, WIDE + half :])
    left, right = jnp.concatenate(left, axis=0), jnp.concatenate(right, axis=0)
    first = jnp.concatenate([left, right], axis=1)
    second = jnp.concatenate(second, axis=0)
    root = math.sqrt(2.0 / math.pi)
    for pair in range(0, LAT, 2):
        hiddens, cots = [], []
        for t in (pair, pair + 1):
            rows = slice(t * WIDE, (t + 1) * WIDE)
            hiddens.append(jnp.concatenate([hidden_ref[i, rows] for i in range(groups)], axis=0))
            cots.append(cot_ref[t])
        hidden = jnp.concatenate(hiddens, axis=1)
        cot = jnp.concatenate(cots, axis=1)
        x = heads_dot(first, hidden)
        back = rows_dot(second, cot)
        square = x * x
        bend = jnp.tanh(root * x * (1.0 + 0.044715 * square))
        half = 0.5 + 0.5 * bend
        slope = half + 0.5 * x * (1.0 - bend * bend) * (root * (1.0 + 3 * 0.044715 * square))
        inner = (slope * back).astype(BF)
        active = (x * half).astype(BF)
        grad = (cot.astype(F32) + rows_dot(first, inner)).astype(BF)
        output = (hidden.astype(F32) + heads_dot(second, active)).astype(BF)
        for at, t in enumerate((pair, pair + 1)):
            lanes = slice(at * LANES, (at + 1) * LANES)
            output_ref[t] = output[:, lanes]
            for i in range(groups):
                grad_ref[i, t * WIDE : (t + 1) * WIDE, :] = grad[i * WIDE : (i + 1) * WIDE, lanes]


def back_dft_kernel(grad_ref, table_ref, mover_ref, send_ref):
    spec = lanes_dot(side_by_side(grad_ref), table_ref[...]).astype(BF)
    send_orders(spec, mover_ref[...], send_ref)


def state_grad_kernel(order_ref, recv_ref, table_ref, mover_ref, grad_ref, out_ref):
    field = take_orders(recv_ref, mover_ref[...], table_ref.shape[0] // 2)
    wave = rows_dot(field, table_ref[...])
    slots = table_ref.shape[0] // 2
    wave = by_latitude(wave, lambda t: order_ref[:, slots + t : slots + t + 1])
    out_ref[...] = (side_by_side(grad_ref).astype(F32) + wave).astype(BF)


def call(kernel, outs, scalars, arrays, flops, name, scratch=(), limit=VMEM_LIMIT):
    out_shape = [jax.ShapeDtypeStruct(s, d) for s, d in outs]
    vmem = pl.BlockSpec(memory_space=pltpu.VMEM)
    smem = pl.BlockSpec(memory_space=pltpu.SMEM)
    single = len(outs) == 1
    moved = sum(a.size * a.dtype.itemsize for a in arrays)
    return pl.pallas_call(
        kernel,
        out_shape=out_shape[0] if single else out_shape,
        in_specs=[smem] * len(scalars) + [vmem] * len(arrays),
        out_specs=vmem if single else [vmem] * len(outs),
        scratch_shapes=[pltpu.VMEM(shape, dtype) for shape, dtype in scratch],
        compiler_params=pltpu.CompilerParams(vmem_limit_bytes=limit),
        cost_estimate=pl.CostEstimate(flops=flops, bytes_accessed=moved, transcendentals=0),
        name=name,
    )(*scalars, *arrays)


def shards(
    state,
    cotangent,
    order_table,
    quad_weight,
    legendre,
    spec_gain,
    spectral_weight,
    mlp_in,
    mlp_out,
):
    lat_rows, chan_width, lon_count = state.shape
    order_count = order_table.shape[0]
    slot_count, degree_rows, lat_count = legendre.shape
    space_count, chan_count = lax.axis_size("space"), lax.axis_size("chan")
    devices = space_count * chan_count
    channels = chan_count * chan_width
    both = ("chan", "space")

    def exchange(rows):
        pieces = rows.reshape(devices * lat_rows // 2, 2, LANES)
        moved = lax.all_to_all(pieces, both, split_axis=0, concat_axis=0, tiled=True)
        return moved.reshape(devices * lat_rows, LANES)

    def cross(blocks):
        return lax.all_to_all(blocks, "chan", split_axis=0, concat_axis=0, tiled=True)

    space_at, chan_at = lax.axis_index("space"), lax.axis_index("chan")
    own_row = jnp.minimum(chan_at, slot_count - 1)
    own = jnp.stack([space_at * slot_count + own_row, own_row])

    per_slot = degree_rows // UNIT
    units = (slot_count + 1) * per_slot + 1
    packed, layers = call(
        pack_kernel,
        [
            ((units, UNIT, lat_count), BF),
            ((mlp_in.shape[0] * 3 // 2 + mlp_out.shape[0], mlp_out.shape[1]), BF),
        ],
        [],
        [legendre.reshape(slot_count * per_slot, UNIT, lat_count), spec_gain, mlp_in, mlp_out],
        1000,
        "pack",
        limit=60 * 1024 * 1024,
    )
    tables = lax.all_gather(packed, "chan", axis=0)
    all_layers = lax.all_gather(layers, "chan", axis=0)
    weight = call(
        build_weight,
        [((2 * channels, 2 * channels), BF)],
        [],
        [spectral_weight],
        2 * 10**9,
        "weight",
    )

    flat = (lat_rows * chan_width, lon_count)
    send = (devices * lat_rows, LANES)
    table_shape = (2 * order_count, lon_count)
    blocks = (chan_count, lat_rows * chan_width, LANES)
    slot_shape = (chan_count, lat_count, LANES)
    dft_flops = 2 * 2 * order_count * lat_rows * chan_width * lon_count
    slot_flops = 2 * order_count * 2 * channels * (2 * lat_count + 2 * channels)
    flat_state = state.reshape(flat)
    order_row = jnp.concatenate([order_table.astype(F32), quad_weight])[None, :]

    table, mover, sent = call(
        dft_kernel,
        [(table_shape, BF), ((LANES * lat_rows, LANES * lat_rows), BF), (send, BF)],
        [],
        [order_row, flat_state],
        dft_flops,
        "dft",
    )
    received = exchange(sent).reshape(slot_shape)
    square = (order_count, lat_count)
    sent, own_legendre, gain = call(
        slot_kernel,
        [(slot_shape, BF), (square, BF), ((order_count, channels), BF)],
        [own, order_table],
        [received, tables, weight],
        slot_flops,
        "slot",
    )
    received = exchange(sent.reshape(send))
    hidden = call(
        hidden_kernel,
        [(blocks, BF)],
        [],
        [received, table, mover, flat_state],
        dft_flops,
        "hidden",
    )
    point_hidden = cross(hidden)
    output, point_grad = call(
        mlp_kernel,
        [(cotangent.shape, BF), (blocks, BF)],
        [],
        [point_hidden, cotangent, all_layers],
        4 * dft_flops,
        "mlp",
    )
    hidden_grad = cross(point_grad)
    sent = call(
        back_dft_kernel, [(send, BF)], [], [hidden_grad, table, mover], dft_flops, "back_dft"
    )
    received = exchange(sent).reshape(slot_shape)
    sent = call(
        back_slot_kernel,
        [(slot_shape, BF)],
        [own, order_table],
        [received, own_legendre, gain, spectral_weight],
        slot_flops,
        "back_slot",
        scratch=[(weight.shape, BF)],
    )
    received = exchange(sent.reshape(send))
    state_grad = call(
        state_grad_kernel,
        [(flat, BF)],
        [],
        [order_row, received, table, mover, hidden_grad],
        dft_flops,
        "state_grad",
    )
    return (output, state_grad.reshape(state.shape))


def solution(mesh):
    placed = (
        P("space", "chan", None),
        P("space", None, "chan"),
        P(),
        P("space"),
        P("space", "chan", None),
        P("chan", None),
        P(),
        P("chan", None),
        P("chan", None),
    )
    return jax.shard_map(
        shards,
        mesh=mesh,
        in_specs=placed,
        out_specs=(P("space", None, "chan"), P("space", "chan", None)),
        check_vma=False,
    )
```

```python
import functools
import math

import jax
import jax.numpy as jnp
from jax import lax
from jax.experimental import pallas as pl
from jax.experimental.pallas import tpu as pltpu
from jax.sharding import PartitionSpec as P

BF = jnp.bfloat16
F32 = jnp.float32
LAT = 6
WIDE = 64
LANES = 128
VMEM_LIMIT = 28 * 1024 * 1024


def rows_dot(a, b):
    return lax.dot_general(a, b, (((1,), (0,)), ((), ())), preferred_element_type=F32)


def lanes_dot(a, b):
    return lax.dot_general(a, b, (((1,), (1,)), ((), ())), preferred_element_type=F32)


def heads_dot(a, b):
    return lax.dot_general(a, b, (((0,), (0,)), ((), ())), preferred_element_type=F32)


def interleaver():
    size = LANES * LAT
    row = lax.broadcasted_iota(jnp.int32, (size, size), 0)
    col = lax.broadcasted_iota(jnp.int32, (size, size), 1)
    wanted = (col & (LANES - 1)) * LAT + (col >> 7)
    return jnp.where(row == wanted, 1.0, 0.0).astype(BF)


def by_latitude(values, factor):
    pieces = [values[t * WIDE : (t + 1) * WIDE] * factor(t) for t in range(LAT)]
    return jnp.concatenate(pieces, axis=0)


def send_orders(spec, mover, send_ref):
    half = spec.shape[1] // 2
    for q in range(half // LANES):
        pieces = []
        for t in range(LAT):
            rows = spec[t * WIDE : (t + 1) * WIDE]
            real = rows[:, q * LANES : (q + 1) * LANES]
            imag = rows[:, half + q * LANES : half + (q + 1) * LANES]
            pieces.append(jnp.concatenate([real, imag], axis=0))
        block = jnp.concatenate(pieces, axis=1)
        step = LANES * LAT
        send_ref[q * step : (q + 1) * step, :] = lanes_dot(mover, block).astype(BF)


def take_orders(recv_ref, mover, half):
    step = LANES * LAT
    blocks = []
    for q in range(half // LANES):
        blocks.append(heads_dot(recv_ref[q * step : (q + 1) * step, :], mover).astype(BF))
    bands = []
    for t in range(LAT):
        lanes = slice(t * LANES, (t + 1) * LANES)
        real = [b[:WIDE, lanes] for b in blocks]
        imag = [b[WIDE:, lanes] for b in blocks]
        bands.append(jnp.concatenate(real + imag, axis=1))
    return jnp.concatenate(bands, axis=0)


def side_by_side(ref):
    return jnp.concatenate([ref[i] for i in range(ref.shape[0])], axis=1)


def pack_kernel(legendre_ref, gain_ref, in_ref, out_ref, slots_ref, layers_ref):
    rows, width = in_ref.shape
    lanes = out_ref.shape[1]
    over, half = width - lanes, rows // 2
    slots_ref[: legendre_ref.shape[0]] = legendre_ref[...]
    layers_ref[:rows] = in_ref[:, :lanes]
    layers_ref[rows : rows + half, :over] = in_ref[:half, lanes:]
    layers_ref[rows : rows + half, over:] = in_ref[half:, lanes:]
    end = rows + half + out_ref.shape[0]
    layers_ref[rows + half : end] = out_ref[...]
    layers_ref[end:] = gain_ref[...].astype(BF)


def build_weight(spectral_ref, weight_ref):
    real, imag = spectral_ref[0], spectral_ref[1]
    groups = real.shape[1] // WIDE

    def paired(left, right):
        pieces = []
        for i in range(groups):
            lanes = slice(i * WIDE, (i + 1) * WIDE)
            pieces += [left[:, lanes], right[:, lanes]]
        return jnp.concatenate(pieces, axis=1)

    for at, rows in enumerate((paired(real, imag), paired(-imag, real))):
        for i in range(groups):
            start = (2 * i + at) * WIDE
            weight_ref[start : start + WIDE] = rows[i * WIDE : (i + 1) * WIDE]


def dft_kernel(order_ref, state_ref, table_ref, mover_ref, send_ref):
    slots = table_ref.shape[0] // 2
    lon_count = state_ref.shape[1]
    spaces = slots // LAT
    place = lax.broadcasted_iota(jnp.int32, (slots, slots), 0)
    wanted = (place & (spaces - 1)) * LAT + place // spaces
    lane = lax.broadcasted_iota(jnp.int32, (slots, slots), 1)
    picked = jnp.where(lane == wanted, order_ref[:, :slots], 0.0)
    orders = jnp.sum(picked, axis=1, keepdims=True).astype(jnp.int32)
    points = lax.broadcasted_iota(jnp.int32, (slots, LANES), 1)
    step = 2.0 * math.pi / lon_count
    factor = 1.0 / math.sqrt(lon_count)
    angles = ((points * orders) & (lon_count - 1)).astype(F32) * step
    turns = ((jnp.full_like(points, LANES) * orders) & (lon_count - 1)).astype(F32) * step
    cosine, sine = jnp.cos(angles) * factor, jnp.sin(angles) * factor
    turn_cos, turn_sin = jnp.cos(turns), jnp.sin(turns)
    for a in range(lon_count // LANES):
        lanes = slice(a * LANES, (a + 1) * LANES)
        table_ref[:slots, lanes] = cosine.astype(BF)
        table_ref[slots:, lanes] = (-sine).astype(BF)
        cosine, sine = (
            cosine * turn_cos - sine * turn_sin,
            sine * turn_cos + cosine * turn_sin,
        )
    mover_ref[...] = interleaver()
    spec = lanes_dot(state_ref[...], table_ref[...])
    spec = by_latitude(spec, lambda t: order_ref[:, slots + t : slots + t + 1]).astype(BF)
    send_orders(spec, mover_ref[...], send_ref)


def gain_lanes(layers_ref, degree_rows):
    start = layers_ref.shape[1] - degree_rows
    groups = layers_ref.shape[0]
    gain = jnp.concatenate([layers_ref[i, start:] for i in range(groups)], axis=0)
    wide = []
    for i in range(groups):
        piece = gain[:, i * WIDE : (i + 1) * WIDE].astype(F32)
        wide.append(jnp.concatenate([piece, piece], axis=1))
    return wide


def slot_scale(own_ref, order_ref):
    return jnp.where(order_ref[own_ref[0]] == 0, 1.0, 2.0).astype(F32)


def slot_kernel(
    own_ref, order_ref, recv_ref, legendre_ref, layers_ref, spectral_ref, send_ref, weight_ref
):
    build_weight(spectral_ref, weight_ref)
    scale = slot_scale(own_ref, order_ref)
    legendre = legendre_ref[...]
    coeffs = rows_dot(legendre, side_by_side(recv_ref)).astype(BF)
    mixed = rows_dot(coeffs, weight_ref[...])
    wide = gain_lanes(layers_ref, legendre.shape[0] // recv_ref.shape[0])
    parts = [
        (mixed[:, i * LANES : (i + 1) * LANES] * wide[i]).astype(BF) for i in range(len(wide))
    ]
    synth = heads_dot(legendre, jnp.concatenate(parts, axis=1)) * scale
    for i in range(len(wide)):
        send_ref[i] = synth[:, i * LANES : (i + 1) * LANES].astype(BF)


def back_slot_kernel(
    own_ref, order_ref, recv_ref, legendre_ref, layers_ref, spectral_ref, send_ref, weight_ref
):
    build_weight(spectral_ref, weight_ref)
    scale = slot_scale(own_ref, order_ref)
    legendre = legendre_ref[...]
    coeffs = (rows_dot(legendre, side_by_side(recv_ref)) * scale).astype(BF).astype(F32)
    wide = gain_lanes(layers_ref, legendre.shape[0] // recv_ref.shape[0])
    scaled = [
        (coeffs[:, i * LANES : (i + 1) * LANES] * wide[i]).astype(BF) for i in range(len(wide))
    ]
    mixed = lanes_dot(jnp.concatenate(scaled, axis=1), weight_ref[...]).astype(BF)
    field = heads_dot(legendre, mixed).astype(BF)
    for i in range(len(wide)):
        send_ref[i] = field[:, i * LANES : (i + 1) * LANES]


def hidden_kernel(recv_ref, table_ref, mover_ref, state_ref, hidden_ref):
    field = take_orders(recv_ref, mover_ref[...], table_ref.shape[0] // 2)
    wave = rows_dot(field, table_ref[...])
    hidden = (state_ref[...].astype(F32) + wave).astype(BF)
    for i in range(hidden_ref.shape[0]):
        hidden_ref[i] = hidden[:, i * LANES : (i + 1) * LANES]


def mlp_kernel(hidden_ref, cot_ref, layers_ref, output_ref, grad_ref):
    groups = hidden_ref.shape[0]
    left, right, second = [], [], []
    half, over, hid = WIDE // 2, layers_ref.shape[2] // 2, (WIDE * 3) // 2
    for i in range(groups):
        left.append(layers_ref[i, :WIDE])
        right.append(layers_ref[i, WIDE : WIDE + half, :over])
        right.append(layers_ref[i, WIDE : WIDE + half, over:])
        second.append(layers_ref[i, WIDE + half : WIDE + half + hid])
    left, right = jnp.concatenate(left, axis=0), jnp.concatenate(right, axis=0)
    first = jnp.concatenate([left, right], axis=1)
    second = jnp.concatenate(second, axis=0)
    root = math.sqrt(2.0 / math.pi)
    for pair in range(0, LAT, 2):
        hiddens, cots = [], []
        for t in (pair, pair + 1):
            rows = slice(t * WIDE, (t + 1) * WIDE)
            hiddens.append(jnp.concatenate([hidden_ref[i, rows] for i in range(groups)], axis=0))
            cots.append(cot_ref[t])
        hidden = jnp.concatenate(hiddens, axis=1)
        cot = jnp.concatenate(cots, axis=1)
        x = heads_dot(first, hidden)
        back = rows_dot(second, cot)
        square = x * x
        bend = jnp.tanh(root * x * (1.0 + 0.044715 * square))
        half = 0.5 + 0.5 * bend
        slope = half + 0.5 * x * (1.0 - bend * bend) * (root * (1.0 + 3 * 0.044715 * square))
        inner = (slope * back).astype(BF)
        active = (x * half).astype(BF)
        grad = (cot.astype(F32) + rows_dot(first, inner)).astype(BF)
        output = (hidden.astype(F32) + heads_dot(second, active)).astype(BF)
        for at, t in enumerate((pair, pair + 1)):
            lanes = slice(at * LANES, (at + 1) * LANES)
            output_ref[t] = output[:, lanes]
            for i in range(groups):
                grad_ref[i, t * WIDE : (t + 1) * WIDE, :] = grad[i * WIDE : (i + 1) * WIDE, lanes]


def back_dft_kernel(grad_ref, table_ref, mover_ref, send_ref):
    spec = lanes_dot(side_by_side(grad_ref), table_ref[...]).astype(BF)
    send_orders(spec, mover_ref[...], send_ref)


def state_grad_kernel(order_ref, recv_ref, table_ref, mover_ref, grad_ref, out_ref):
    field = take_orders(recv_ref, mover_ref[...], table_ref.shape[0] // 2)
    wave = rows_dot(field, table_ref[...])
    slots = table_ref.shape[0] // 2
    wave = by_latitude(wave, lambda t: order_ref[:, slots + t : slots + t + 1])
    out_ref[...] = (side_by_side(grad_ref).astype(F32) + wave).astype(BF)


def call(kernel, outs, scalars, arrays, flops, name, scratch=(), limit=VMEM_LIMIT):
    out_shape = [jax.ShapeDtypeStruct(s, d) for s, d in outs]
    vmem = pl.BlockSpec(memory_space=pltpu.VMEM)
    smem = pl.BlockSpec(memory_space=pltpu.SMEM)
    single = len(outs) == 1
    moved = sum(a.size * a.dtype.itemsize for a in arrays)
    return pl.pallas_call(
        kernel,
        out_shape=out_shape[0] if single else out_shape,
        in_specs=[smem] * len(scalars) + [vmem] * len(arrays),
        out_specs=vmem if single else [vmem] * len(outs),
        scratch_shapes=[pltpu.VMEM(shape, dtype) for shape, dtype in scratch],
        compiler_params=pltpu.CompilerParams(vmem_limit_bytes=limit),
        cost_estimate=pl.CostEstimate(flops=flops, bytes_accessed=moved, transcendentals=0),
        name=name,
    )(*scalars, *arrays)


def shards(
    state,
    cotangent,
    order_table,
    quad_weight,
    legendre,
    spec_gain,
    spectral_weight,
    mlp_in,
    mlp_out,
):
    lat_rows, chan_width, lon_count = state.shape
    order_count = order_table.shape[0]
    slot_count, degree_rows, lat_count = legendre.shape
    space_count, chan_count = lax.axis_size("space"), lax.axis_size("chan")
    devices = space_count * chan_count
    channels = chan_count * chan_width
    both = ("chan", "space")

    def exchange(rows):
        pieces = rows.reshape(devices * lat_rows // 2, 2, LANES)
        moved = lax.all_to_all(pieces, both, split_axis=0, concat_axis=0, tiled=True)
        return moved.reshape(devices * lat_rows, LANES)

    def cross(blocks):
        return lax.all_to_all(blocks, "chan", split_axis=0, concat_axis=0, tiled=True)

    space_at, chan_at = lax.axis_index("space"), lax.axis_index("chan")
    own_row = jnp.minimum(chan_at, slot_count - 1)
    own = jnp.stack([space_at * slot_count + own_row, own_row])

    layer_rows = mlp_in.shape[0] * 3 // 2 + mlp_out.shape[0] + degree_rows
    slots, layers = call(
        pack_kernel,
        [
            ((chan_count, degree_rows, lat_count), BF),
            ((layer_rows, mlp_out.shape[1]), BF),
        ],
        [],
        [legendre, spec_gain, mlp_in, mlp_out],
        1000,
        "pack",
        limit=60 * 1024 * 1024,
    )
    all_layers = lax.all_gather(layers, "chan", axis=0)
    own_legendre = cross(slots).reshape(order_count, lat_count)

    flat = (lat_rows * chan_width, lon_count)
    send = (devices * lat_rows, LANES)
    table_shape = (2 * order_count, lon_count)
    blocks = (chan_count, lat_rows * chan_width, LANES)
    slot_shape = (chan_count, lat_count, LANES)
    dft_flops = 2 * 2 * order_count * lat_rows * chan_width * lon_count
    slot_flops = 2 * order_count * 2 * channels * (2 * lat_count + 2 * channels)
    flat_state = state.reshape(flat)
    order_row = jnp.concatenate([order_table.astype(F32), quad_weight])[None, :]

    table, mover, sent = call(
        dft_kernel,
        [(table_shape, BF), ((LANES * lat_rows, LANES * lat_rows), BF), (send, BF)],
        [],
        [order_row, flat_state],
        dft_flops,
        "dft",
    )
    received = exchange(sent).reshape(slot_shape)
    square = (2 * channels, 2 * channels)
    sent = call(
        slot_kernel,
        [(slot_shape, BF)],
        [own, order_table],
        [received, own_legendre, all_layers, spectral_weight],
        slot_flops,
        "slot",
        scratch=[(square, BF)],
    )
    received = exchange(sent.reshape(send))
    hidden = call(
        hidden_kernel,
        [(blocks, BF)],
        [],
        [received, table, mover, flat_state],
        dft_flops,
        "hidden",
    )
    point_hidden = cross(hidden)
    output, point_grad = call(
        mlp_kernel,
        [(cotangent.shape, BF), (blocks, BF)],
        [],
        [point_hidden, cotangent, all_layers],
        4 * dft_flops,
        "mlp",
    )
    hidden_grad = cross(point_grad)
    sent = call(
        back_dft_kernel, [(send, BF)], [], [hidden_grad, table, mover], dft_flops, "back_dft"
    )
    received = exchange(sent).reshape(slot_shape)
    sent = call(
        back_slot_kernel,
        [(slot_shape, BF)],
        [own, order_table],
        [received, own_legendre, all_layers, spectral_weight],
        slot_flops,
        "back_slot",
        scratch=[(square, BF)],
    )
    received = exchange(sent.reshape(send))
    state_grad = call(
        state_grad_kernel,
        [(flat, BF)],
        [],
        [order_row, received, table, mover, hidden_grad],
        dft_flops,
        "state_grad",
    )
    return (output, state_grad.reshape(state.shape))


def solution(mesh):
    placed = (
        P("space", "chan", None),
        P("space", None, "chan"),
        P(),
        P("space"),
        P("space", "chan", None),
        P("chan", None),
        P(),
        P("chan", None),
        P("chan", None),
    )
    return jax.shard_map(
        shards,
        mesh=mesh,
        in_specs=placed,
        out_specs=(P("space", None, "chan"), P("space", "chan", None)),
        check_vma=False,
    )
```

```python
import functools
import math

import jax
import jax.numpy as jnp
from jax import lax
from jax.experimental import pallas as pl
from jax.experimental.pallas import tpu as pltpu
from jax.sharding import PartitionSpec as P

BF = jnp.bfloat16
F32 = jnp.float32
LAT = 6
WIDE = 64
LANES = 128
VMEM_LIMIT = 28 * 1024 * 1024


def rows_dot(a, b):
    return lax.dot_general(a, b, (((1,), (0,)), ((), ())), preferred_element_type=F32)


def lanes_dot(a, b):
    return lax.dot_general(a, b, (((1,), (1,)), ((), ())), preferred_element_type=F32)


def heads_dot(a, b):
    return lax.dot_general(a, b, (((0,), (0,)), ((), ())), preferred_element_type=F32)


def interleaver():
    size = LANES * LAT
    row = lax.broadcasted_iota(jnp.int32, (size, size), 0)
    col = lax.broadcasted_iota(jnp.int32, (size, size), 1)
    wanted = (col & (LANES - 1)) * LAT + (col >> 7)
    return jnp.where(row == wanted, 1.0, 0.0).astype(BF)


def by_latitude(values, factor):
    pieces = [values[t * WIDE : (t + 1) * WIDE] * factor(t) for t in range(LAT)]
    return jnp.concatenate(pieces, axis=0)


def send_orders(spec, mover, send_ref):
    half = spec.shape[1] // 2
    for q in range(half // LANES):
        pieces = []
        for t in range(LAT):
            rows = spec[t * WIDE : (t + 1) * WIDE]
            real = rows[:, q * LANES : (q + 1) * LANES]
            imag = rows[:, half + q * LANES : half + (q + 1) * LANES]
            pieces.append(jnp.concatenate([real, imag], axis=0))
        block = jnp.concatenate(pieces, axis=1)
        step = LANES * LAT
        send_ref[q * step : (q + 1) * step, :] = lanes_dot(mover, block).astype(BF)


def take_orders(recv_ref, mover, half):
    step = LANES * LAT
    blocks = []
    for q in range(half // LANES):
        blocks.append(heads_dot(recv_ref[q * step : (q + 1) * step, :], mover).astype(BF))
    bands = []
    for t in range(LAT):
        lanes = slice(t * LANES, (t + 1) * LANES)
        real = [b[:WIDE, lanes] for b in blocks]
        imag = [b[WIDE:, lanes] for b in blocks]
        bands.append(jnp.concatenate(real + imag, axis=1))
    return jnp.concatenate(bands, axis=0)


def side_by_side(ref):
    return jnp.concatenate([ref[i] for i in range(ref.shape[0])], axis=1)


def pack_kernel(legendre_ref, gain_ref, in_ref, out_ref, slots_ref, layers_ref):
    rows, width = in_ref.shape
    lanes = out_ref.shape[1]
    over, half = width - lanes, rows // 2
    slots_ref[: legendre_ref.shape[0]] = legendre_ref[...]
    layers_ref[:rows] = in_ref[:, :lanes]
    layers_ref[rows : rows + half, :over] = in_ref[:half, lanes:]
    layers_ref[rows : rows + half, over:] = in_ref[half:, lanes:]
    end = rows + half + out_ref.shape[0]
    layers_ref[rows + half : end] = out_ref[...]
    layers_ref[end:] = gain_ref[...].astype(BF)


def build_weight(spectral_ref, weight_ref):
    real, imag = spectral_ref[0], spectral_ref[1]
    groups = real.shape[1] // WIDE

    def paired(left, right):
        pieces = []
        for i in range(groups):
            lanes = slice(i * WIDE, (i + 1) * WIDE)
            pieces += [left[:, lanes], right[:, lanes]]
        return jnp.concatenate(pieces, axis=1)

    for at, rows in enumerate((paired(real, imag), paired(-imag, real))):
        for i in range(groups):
            start = (2 * i + at) * WIDE
            weight_ref[start : start + WIDE] = rows[i * WIDE : (i + 1) * WIDE]


def dft_kernel(own_ref, order_ref, state_ref, table_ref, mover_ref, send_ref):
    slots = table_ref.shape[0] // 2
    lon_count = state_ref.shape[1]
    spaces = slots // LAT
    place = lax.broadcasted_iota(jnp.int32, (slots, slots), 0)
    wanted = (place & (spaces - 1)) * LAT + place // spaces
    lane = lax.broadcasted_iota(jnp.int32, (slots, slots), 1)
    picked = jnp.where(lane == wanted, order_ref[:, :slots], 0.0)
    orders = jnp.sum(picked, axis=1, keepdims=True).astype(jnp.int32)
    points = lax.broadcasted_iota(jnp.int32, (slots, LANES), 1)
    step = 2.0 * math.pi / lon_count
    factor = 1.0 / math.sqrt(lon_count)
    angles = ((points * orders) & (lon_count - 1)).astype(F32) * step
    turns = ((jnp.full_like(points, LANES) * orders) & (lon_count - 1)).astype(F32) * step
    cosine, sine = jnp.cos(angles) * factor, jnp.sin(angles) * factor
    turn_cos, turn_sin = jnp.cos(turns), jnp.sin(turns)
    for a in range(lon_count // LANES):
        lanes = slice(a * LANES, (a + 1) * LANES)
        table_ref[:slots, lanes] = cosine.astype(BF)
        table_ref[slots:, lanes] = (-sine).astype(BF)
        cosine, sine = (
            cosine * turn_cos - sine * turn_sin,
            sine * turn_cos + cosine * turn_sin,
        )
    mover_ref[...] = interleaver()
    spec = lanes_dot(state_ref[...], table_ref[...])
    spec = by_latitude(spec, lambda t: order_ref[:, slots + t : slots + t + 1]).astype(BF)
    send_orders(spec, mover_ref[...], send_ref)


def gain_lanes(layers_ref, degree_rows):
    start = layers_ref.shape[1] - degree_rows
    groups = layers_ref.shape[0]
    gain = jnp.concatenate([layers_ref[i, start:] for i in range(groups)], axis=0)
    wide = []
    for i in range(groups):
        piece = gain[:, i * WIDE : (i + 1) * WIDE].astype(F32)
        wide.append(jnp.concatenate([piece, piece], axis=1))
    return wide


def slot_scale(own_ref, order_ref):
    return jnp.where(order_ref[own_ref[0]] == 0, 1.0, 2.0).astype(F32)


def slot_kernel(
    own_ref, order_ref, recv_ref, legendre_ref, layers_ref, spectral_ref, send_ref, weight_ref
):
    build_weight(spectral_ref, weight_ref)
    scale = slot_scale(own_ref, order_ref)
    legendre = legendre_ref[...]
    coeffs = rows_dot(legendre, side_by_side(recv_ref)).astype(BF)
    mixed = rows_dot(coeffs, weight_ref[...])
    wide = gain_lanes(layers_ref, legendre.shape[0] // recv_ref.shape[0])
    parts = [
        (mixed[:, i * LANES : (i + 1) * LANES] * wide[i]).astype(BF) for i in range(len(wide))
    ]
    synth = heads_dot(legendre, jnp.concatenate(parts, axis=1)) * scale
    for i in range(len(wide)):
        send_ref[i] = synth[:, i * LANES : (i + 1) * LANES].astype(BF)


def back_slot_kernel(
    own_ref, order_ref, recv_ref, legendre_ref, layers_ref, spectral_ref, send_ref, weight_ref
):
    build_weight(spectral_ref, weight_ref)
    scale = slot_scale(own_ref, order_ref)
    legendre = legendre_ref[...]
    coeffs = (rows_dot(legendre, side_by_side(recv_ref)) * scale).astype(BF).astype(F32)
    wide = gain_lanes(layers_ref, legendre.shape[0] // recv_ref.shape[0])
    scaled = [
        (coeffs[:, i * LANES : (i + 1) * LANES] * wide[i]).astype(BF) for i in range(len(wide))
    ]
    mixed = lanes_dot(jnp.concatenate(scaled, axis=1), weight_ref[...]).astype(BF)
    field = heads_dot(legendre, mixed).astype(BF)
    for i in range(len(wide)):
        send_ref[i] = field[:, i * LANES : (i + 1) * LANES]


def hidden_kernel(recv_ref, table_ref, mover_ref, state_ref, hidden_ref):
    field = take_orders(recv_ref, mover_ref[...], table_ref.shape[0] // 2)
    wave = rows_dot(field, table_ref[...])
    hidden = (state_ref[...].astype(F32) + wave).astype(BF)
    for i in range(hidden_ref.shape[0]):
        hidden_ref[i] = hidden[:, i * LANES : (i + 1) * LANES]


def mlp_kernel(hidden_ref, cot_ref, layers_ref, output_ref, grad_ref):
    groups = hidden_ref.shape[0]
    left, right, second = [], [], []
    half, over, hid = WIDE // 2, layers_ref.shape[2] // 2, (WIDE * 3) // 2
    for i in range(groups):
        left.append(layers_ref[i, :WIDE])
        right.append(layers_ref[i, WIDE : WIDE + half, :over])
        right.append(layers_ref[i, WIDE : WIDE + half, over:])
        second.append(layers_ref[i, WIDE + half : WIDE + half + hid])
    left, right = jnp.concatenate(left, axis=0), jnp.concatenate(right, axis=0)
    first = jnp.concatenate([left, right], axis=1)
    second = jnp.concatenate(second, axis=0)
    root = math.sqrt(2.0 / math.pi)
    for pair in range(0, LAT, 2):
        hiddens, cots = [], []
        for t in (pair, pair + 1):
            rows = slice(t * WIDE, (t + 1) * WIDE)
            hiddens.append(jnp.concatenate([hidden_ref[i, rows] for i in range(groups)], axis=0))
            cots.append(cot_ref[t])
        hidden = jnp.concatenate(hiddens, axis=1)
        cot = jnp.concatenate(cots, axis=1)
        x = heads_dot(first, hidden)
        back = rows_dot(second, cot)
        square = x * x
        bend = jnp.tanh(root * x * (1.0 + 0.044715 * square))
        half = 0.5 + 0.5 * bend
        slope = half + 0.5 * x * (1.0 - bend * bend) * (root * (1.0 + 3 * 0.044715 * square))
        inner = (slope * back).astype(BF)
        active = (x * half).astype(BF)
        grad = (cot.astype(F32) + rows_dot(first, inner)).astype(BF)
        output = (hidden.astype(F32) + heads_dot(second, active)).astype(BF)
        for at, t in enumerate((pair, pair + 1)):
            lanes = slice(at * LANES, (at + 1) * LANES)
            output_ref[t] = output[:, lanes]
            for i in range(groups):
                grad_ref[i, t * WIDE : (t + 1) * WIDE, :] = grad[i * WIDE : (i + 1) * WIDE, lanes]


def back_dft_kernel(grad_ref, table_ref, mover_ref, send_ref):
    spec = lanes_dot(side_by_side(grad_ref), table_ref[...]).astype(BF)
    send_orders(spec, mover_ref[...], send_ref)


def state_grad_kernel(order_ref, recv_ref, table_ref, mover_ref, grad_ref, out_ref):
    field = take_orders(recv_ref, mover_ref[...], table_ref.shape[0] // 2)
    wave = rows_dot(field, table_ref[...])
    slots = table_ref.shape[0] // 2
    wave = by_latitude(wave, lambda t: order_ref[:, slots + t : slots + t + 1])
    out_ref[...] = (side_by_side(grad_ref).astype(F32) + wave).astype(BF)


def call(kernel, outs, scalars, arrays, flops, name, scratch=(), limit=VMEM_LIMIT):
    out_shape = [jax.ShapeDtypeStruct(s, d) for s, d in outs]
    vmem = pl.BlockSpec(memory_space=pltpu.VMEM)
    smem = pl.BlockSpec(memory_space=pltpu.SMEM)
    single = len(outs) == 1
    moved = sum(a.size * a.dtype.itemsize for a in arrays)
    return pl.pallas_call(
        kernel,
        out_shape=out_shape[0] if single else out_shape,
        in_specs=[smem] * len(scalars) + [vmem] * len(arrays),
        out_specs=vmem if single else [vmem] * len(outs),
        scratch_shapes=[pltpu.VMEM(shape, dtype) for shape, dtype in scratch],
        compiler_params=pltpu.CompilerParams(vmem_limit_bytes=limit),
        cost_estimate=pl.CostEstimate(flops=flops, bytes_accessed=moved, transcendentals=0),
        name=name,
    )(*scalars, *arrays)


def shards(
    state,
    cotangent,
    order_table,
    quad_weight,
    legendre,
    spec_gain,
    spectral_weight,
    mlp_in,
    mlp_out,
):
    lat_rows, chan_width, lon_count = state.shape
    order_count = order_table.shape[0]
    slot_count, degree_rows, lat_count = legendre.shape
    space_count, chan_count = lax.axis_size("space"), lax.axis_size("chan")
    devices = space_count * chan_count
    channels = chan_count * chan_width
    both = ("chan", "space")

    def exchange(rows):
        pieces = rows.reshape(devices * lat_rows // 2, 2, LANES)
        moved = lax.all_to_all(pieces, both, split_axis=0, concat_axis=0, tiled=True)
        return moved.reshape(devices * lat_rows, LANES)

    def cross(blocks):
        return lax.all_to_all(blocks, "chan", split_axis=0, concat_axis=0, tiled=True)

    space_at, chan_at = lax.axis_index("space"), lax.axis_index("chan")
    own_row = jnp.minimum(chan_at, slot_count - 1)
    own = jnp.stack([space_at * slot_count + own_row, own_row])

    layer_rows = mlp_in.shape[0] * 3 // 2 + mlp_out.shape[0] + degree_rows
    slots, layers = call(
        pack_kernel,
        [
            ((chan_count, degree_rows, lat_count), BF),
            ((layer_rows, mlp_out.shape[1]), BF),
        ],
        [],
        [legendre, spec_gain, mlp_in, mlp_out],
        1000,
        "pack",
        limit=60 * 1024 * 1024,
    )
    all_layers = lax.all_gather(layers, "chan", axis=0)
    own_legendre = cross(slots).reshape(order_count, lat_count)

    flat = (lat_rows * chan_width, lon_count)
    send = (devices * lat_rows, LANES)
    table_shape = (2 * order_count, lon_count)
    blocks = (chan_count, lat_rows * chan_width, LANES)
    slot_shape = (chan_count, lat_count, LANES)
    dft_flops = 2 * 2 * order_count * lat_rows * chan_width * lon_count
    slot_flops = 2 * order_count * 2 * channels * (2 * lat_count + 2 * channels)
    flat_state = state.reshape(flat)
    order_row = jnp.concatenate([order_table.astype(F32), quad_weight])[None, :]

    table, mover, sent = call(
        dft_kernel,
        [(table_shape, BF), ((LANES * lat_rows, LANES * lat_rows), BF), (send, BF)],
        [own],
        [order_row, flat_state],
        dft_flops,
        "dft",
    )
    received = exchange(sent).reshape(slot_shape)
    square = (2 * channels, 2 * channels)
    sent = call(
        slot_kernel,
        [(slot_shape, BF)],
        [own, order_table],
        [received, own_legendre, all_layers, spectral_weight],
        slot_flops,
        "slot",
        scratch=[(square, BF)],
    )
    received = exchange(sent.reshape(send))
    hidden = call(
        hidden_kernel,
        [(blocks, BF)],
        [],
        [received, table, mover, flat_state],
        dft_flops,
        "hidden",
    )
    point_hidden = cross(hidden)
    output, point_grad = call(
        mlp_kernel,
        [(cotangent.shape, BF), (blocks, BF)],
        [],
        [point_hidden, cotangent, all_layers],
        4 * dft_flops,
        "mlp",
    )
    hidden_grad = cross(point_grad)
    sent = call(
        back_dft_kernel, [(send, BF)], [], [hidden_grad, table, mover], dft_flops, "back_dft"
    )
    received = exchange(sent).reshape(slot_shape)
    sent = call(
        back_slot_kernel,
        [(slot_shape, BF)],
        [own, order_table],
        [received, own_legendre, all_layers, spectral_weight],
        slot_flops,
        "back_slot",
        scratch=[(square, BF)],
    )
    received = exchange(sent.reshape(send))
    state_grad = call(
        state_grad_kernel,
        [(flat, BF)],
        [],
        [order_row, received, table, mover, hidden_grad],
        dft_flops,
        "state_grad",
    )
    return (output, state_grad.reshape(state.shape))


def solution(mesh):
    placed = (
        P("space", "chan", None),
        P("space", None, "chan"),
        P(),
        P("space"),
        P("space", "chan", None),
        P("chan", None),
        P(),
        P("chan", None),
        P("chan", None),
    )
    return jax.shard_map(
        shards,
        mesh=mesh,
        in_specs=placed,
        out_specs=(P("space", None, "chan"), P("space", "chan", None)),
        check_vma=False,
    )
```
